32 devices in a mesh: dp: 16 (over z, x, core), mp: 2 (over y).
Axes of the slice: x: 2, y: 2, z: 4, core: 2. Of those that a mesh axis runs over, the one named last changes fastest.
Arguments:
- tokens: bfloat16 [8192, 8192], P('dp'), may hold values from -6 to 6
- queries: bfloat16 [8192, 64, 128], P('dp', 'mp'), may hold values from -68 to 68
- out_grad: bfloat16 [8192, 64, 128], P('dp', 'mp'), may hold values from -6 to 6
- segment_ids: int32 [16, 512], P('dp'), may hold values from 0 to 3, never falling along the last dimension, each value on 1 to 256 neighbouring positions
- weight_slots: bfloat16 [16384, 8, 2, 128], P('dp', 'mp'), may hold values from -0.0625 to 0.0625
- old_place: int32 [64], replicated, may hold values from 0 to 127, as said below
- new_place: int32 [64], replicated, may hold values from 0 to 127, as said below
Outputs:
- input_grad: bfloat16 [8192, 8192], P('dp', 'mp')
- query_grad: bfloat16 [8192, 64, 128], P('dp', 'mp')
- weight_grad: float32 [16384, 8, 2, 128], P('dp', 'mp')
The draws below stay inside these ranges and needn't reach their ends.
Inputs may be any that keep to these rules, and one draw needn't show every extreme that they name: `old_place`: entries are distinct slot numbers; slot s lies on index s // 8 of dp; some index of dp holds 8 blocks. `new_place`: entries are distinct slot numbers; slot s lies on index s // 8 of dp; some index of dp receives 8 blocks.
All inputs are finite; a program needn't handle non-finite values.
Results may differ from the reference program's by a relative error of at most 0.018.
Values may be sent and summed in bfloat16 or wider, within the bound.
No kernel may reach another device: no remote copies, remote signals or barrier semaphores. Data moves between devices by JAX's collectives and lax.ppermute only.
A program may use at most 192 MiB of HBM per device.

```python
import math
import jax
import jax.numpy as jnp
import numpy as np
from jax import lax

D = 8192
QH = 64
KVH = 8
HD = 128
BR = 128
TOK = 512
BLOCKS = 64
SLOTS = 8
TOKENS = 8192
N_DP = 16


def place_blocks(key):
    slot_count = N_DP * SLOTS
    first_key, second_key = jax.random.split(key)
    shuffled = jax.random.permutation(first_key, slot_count).astype(jnp.int32)
    busiest = jax.random.randint(second_key, (), 0, N_DP).astype(jnp.int32)
    owner_dev = jnp.arange(slot_count, dtype=jnp.int32) // SLOTS
    priority = shuffled - (owner_dev == busiest).astype(jnp.int32) * slot_count
    ordered = jnp.argsort(priority, stable=True).astype(jnp.int32)
    return ordered[:BLOCKS]


def draw_old_place(key, part):
    return place_blocks(jax.random.fold_in(key, 11))


def draw_new_place(key, part):
    return place_blocks(jax.random.fold_in(key, 23))


def draw_queries(key, part):
    base_key = jax.random.fold_in(key, 0)
    base = jnp.clip(jax.random.normal(base_key, (TOKENS, QH, HD), jnp.float32), -6.0, 6.0)
    return base.astype(jnp.bfloat16)


def strengthened(drawn, own_key, source, target, blocks, factor):
    owner, partner = [(jnp.arange(drawn.shape[axis_at]) // (drawn.shape[axis_at] // blocks)).reshape([-1 if axis == axis_at else 1 for axis in range(drawn.ndim)]) for axis_at in (source, target)]
    chosen = jax.random.permutation(own_key, blocks)[partner]
    strong = (owner == chosen) | (owner == (partner + blocks // 2) % blocks)
    return jnp.where(strong, factor * drawn, drawn)


def block_scale(own_key, extent, cuts, smallest, top_value):
    level = 1.0
    for dim, parts in cuts:
        heights = jax.random.uniform(jax.random.fold_in(jax.random.fold_in(own_key, 6), dim), (parts,), jnp.float32, smallest / len(cuts), top_value / len(cuts))
        level = level * jnp.repeat(jnp.exp(heights), extent[dim] // parts).reshape((-1,) + (1,) * (len(extent) - 1 - dim))
    return level


def length_profile(number_of, total, reach, skew):
    portions = [(1 << 20) // math.isqrt(standing ** skew) + 1 for standing in range(2, number_of + 1)]
    rest, given = total - reach - (number_of - 1), [1] * (number_of - 1)
    while rest > 0:
        candidates = [i for i in range(number_of - 1) if given[i] < reach]
        whole, budget = sum([portions[i] for i in candidates]), rest
        for i in candidates:
            more = min(reach - given[i], max(1, budget * portions[i] // whole), rest)
            given[i] = given[i] + more
            rest = rest - more
    return np.array([reach] + given)


def uneven_parts(key, count, total, bound, slope):
    if count == 2:
        one = jax.random.randint(key, (), max(1, total - bound), min(bound, total - 1) + 1)
        return jnp.stack([one, total - one])
    sizes = jnp.asarray(length_profile(count, total, bound, slope), jnp.int32)
    pairs = (count - 1) // 2
    source_of, taker = sizes[1:1 + 2 * pairs:2], sizes[2:2 + 2 * pairs:2]
    margin = jnp.minimum(source_of - 1, bound - taker)
    moved = jax.random.randint(jax.random.fold_in(key, 1), (pairs,), 0, 1 << 20) % (margin + 1)
    sizes = sizes.at[1:1 + 2 * pairs:2].set(source_of - moved).at[2:2 + 2 * pairs:2].set(taker + moved)
    return sizes[jax.random.permutation(jax.random.fold_in(key, 2), count)]


def centred(rng, shape, spread, reach, cuts=(), kind=jnp.bfloat16):
    gain = block_scale(rng, shape, cuts, -0.22, 0.18) if cuts else 1.0
    array = jax.random.normal(rng, shape, jnp.float32) * spread * gain
    return jnp.minimum(jnp.maximum(array, -reach), reach).astype(kind)


def heavy_noise(rng, shape, width, reach, cuts, heavy, kind=jnp.bfloat16):
    entries = width * jax.random.normal(rng, shape, jnp.float32)
    if cuts:
        entries = entries * block_scale(rng, shape, cuts, -0.22, 0.18)
    return jnp.clip(strengthened(entries, jax.random.fold_in(rng, 3), *heavy), -reach, reach).astype(kind)


def setup_inputs(seed: int = 0) -> dict:
    streams_of = jax.random.split(jax.random.key(seed), 8)
    tokens = heavy_noise(streams_of[0], (TOKENS, D), 1.0, 6.0, ((0, 16),), (0, 1, 16, 2.0))
    queries = draw_queries(jax.random.fold_in(streams_of[7], 71), 0)
    out_grad = centred(streams_of[2], (TOKENS, QH, HD), 1.0, 6.0, ((0, 16), (1, 2)))
    segment_ids = jax.vmap(lambda own: jnp.searchsorted(jnp.cumsum(uneven_parts(own, 4, TOK, TOK // 2, 0)), jnp.arange(TOK), side="right"))(jax.random.split(streams_of[3], N_DP)).reshape((N_DP, TOK)).astype(jnp.int32)
    weight_slots = centred(streams_of[4], (N_DP * SLOTS * BR, KVH, 2, HD), D ** -0.5, 0.0625, ((0, 16), (1, 2)))
    old_place = draw_old_place(jax.random.fold_in(streams_of[7], 71), 0)
    new_place = draw_new_place(jax.random.fold_in(streams_of[7], 71), 0)
    return dict(tokens=tokens, queries=queries, out_grad=out_grad, segment_ids=segment_ids, weight_slots=weight_slots, old_place=old_place, new_place=new_place)


def attend(tokens, weights, queries, out_grad, seg_row):
    tok_count = tokens.shape[0]
    model_width = weights.shape[0]
    head_count = weights.shape[1]
    head_size = weights.shape[3]
    per_head = queries.shape[1] // head_count
    half_size = head_size // 2
    projected = jnp.dot(tokens, weights.reshape(model_width, head_count * 2 * head_size), preferred_element_type=jnp.float32)
    projected = projected.reshape(tok_count, head_count, 2, head_size)
    frequency = 500000.0 ** (-2.0 * jnp.arange(half_size, dtype=jnp.float32) / head_size)
    angle_tab = jnp.arange(tok_count, dtype=jnp.float32)[:, None] * frequency[None, :]
    cos_tab = jnp.cos(angle_tab)[:, None, :]
    sin_tab = jnp.sin(angle_tab)[:, None, :]
    lower_half = projected[:, :, 0, :half_size]
    upper_half = projected[:, :, 0, half_size:]
    rot_keys = jnp.concatenate([lower_half * cos_tab - upper_half * sin_tab, upper_half * cos_tab + lower_half * sin_tab], axis=-1).astype(jnp.bfloat16)
    values = projected[:, :, 1].astype(jnp.bfloat16)
    inv_root = 1.0 / jnp.sqrt(jnp.float32(head_size))
    query_wide = queries.reshape(tok_count, head_count, per_head, head_size).astype(jnp.float32)
    outgrad_wide = out_grad.reshape(tok_count, head_count, per_head, head_size).astype(jnp.float32)
    key_wide = rot_keys.astype(jnp.float32)
    value_wide = values.astype(jnp.float32)
    scores = jnp.einsum('qhgd,khd->hgqk', query_wide, key_wide) * inv_root
    position = jnp.arange(tok_count)
    allowed = (position[:, None] >= position[None, :]) & (seg_row[:, None] == seg_row[None, :])
    scores = jnp.where(allowed, scores, jnp.float32(-1e+30))
    row_max = lax.optimization_barrier(jnp.max(scores, axis=-1, keepdims=True))
    exp_scores = jnp.exp(scores - row_max)
    attn_prob = exp_scores / lax.optimization_barrier(jnp.sum(exp_scores, axis=-1, keepdims=True))
    prob_half = lax.optimization_barrier(attn_prob.astype(jnp.bfloat16)).astype(jnp.float32)
    attn_out = jnp.einsum('hgqk,khd->qhgd', prob_half, value_wide)
    row_dot = lax.optimization_barrier(jnp.sum(outgrad_wide * attn_out, axis=-1))
    prob_grad = jnp.einsum('qhgd,khd->hgqk', outgrad_wide, value_wide)
    score_grad = attn_prob * (prob_grad - jnp.transpose(row_dot, (1, 2, 0))[..., None])
    score_half = lax.optimization_barrier(score_grad.astype(jnp.bfloat16)).astype(jnp.float32)
    query_grad = (jnp.einsum('hgqk,khd->qhgd', score_half, key_wide) * inv_root).reshape(tok_count, head_count * per_head, head_size).astype(jnp.bfloat16)
    rot_grad = jnp.einsum('hgqk,qhgd->khd', score_half, query_wide) * inv_root
    value_grad = jnp.einsum('hgqk,qhgd->khd', prob_half, outgrad_wide)
    grad_lower = rot_grad[..., :half_size]
    grad_upper = rot_grad[..., half_size:]
    key_grad = jnp.concatenate([grad_lower * cos_tab + grad_upper * sin_tab, grad_upper * cos_tab - grad_lower * sin_tab], axis=-1)
    pair_grad = jnp.stack([key_grad, value_grad], axis=2).astype(jnp.bfloat16)
    return (query_grad, pair_grad)

def reference(tokens, queries, out_grad, segment_ids, weight_slots, old_place, new_place):
    in_block = jnp.arange(BR, dtype=jnp.int32)
    old_index = (old_place.astype(jnp.int32)[:, None] * BR + in_block[None, :]).reshape(-1)
    weights = jnp.take(weight_slots, old_index, axis=0)
    weight_flat = weights.reshape(D, KVH * 2 * HD)

    def per_sequence(grad_acc, inputs):
        seq_tokens, seq_queries, seq_outgrad, seq_ids = inputs
        query_grad, pair_grad = attend(seq_tokens, weights, seq_queries, seq_outgrad, seq_ids)
        pair_flat = pair_grad.reshape(TOK, KVH * 2 * HD)
        seq_part = lax.dot_general(seq_tokens, pair_flat, (((0,), (0,)), ((), ())), preferred_element_type=jnp.float32).astype(jnp.bfloat16)
        grad_acc = grad_acc + lax.optimization_barrier(seq_part).astype(jnp.float32)
        input_grad = lax.dot_general(pair_flat, weight_flat, (((1,), (1,)), ((), ())), preferred_element_type=jnp.float32).astype(jnp.bfloat16)
        return (grad_acc, (input_grad, query_grad))
    stacked = (tokens.reshape(N_DP, TOK, D), queries.reshape(N_DP, TOK, QH, HD), out_grad.reshape(N_DP, TOK, QH, HD), segment_ids)
    grad_sum, (input_grads, query_grads) = lax.scan(per_sequence, jnp.zeros((D, KVH * 2 * HD), jnp.float32), stacked)
    slot_ids = jnp.arange(N_DP * SLOTS, dtype=jnp.int32)
    matched = (new_place.astype(jnp.int32)[None, :] == slot_ids[:, None]).astype(jnp.int32)
    slot_block = lax.optimization_barrier(jnp.sum(matched * jnp.arange(BLOCKS, dtype=jnp.int32)[None, :], axis=1))
    slot_used = lax.optimization_barrier(jnp.sum(matched, axis=1)).astype(jnp.float32)
    row_index = (slot_block[:, None] * BR + in_block[None, :]).reshape(-1)
    row_keep = jnp.repeat(slot_used, BR)
    weight_grad = jnp.take(grad_sum, row_index, axis=0) * row_keep[:, None]
    return (input_grads.reshape(TOKENS, D), query_grads.reshape(TOKENS, QH, HD), weight_grad.reshape(N_DP * SLOTS * BR, KVH, 2, HD))
```

```python
import functools

import jax
import jax.numpy as jnp
from jax import lax
from jax.experimental import pallas as pl
from jax.experimental.pallas import tpu as pltpu
from jax.sharding import PartitionSpec as P

BR = 128
QT = 128
REACH = 2
NEG = -1e30


def attn_kernel(proj_ref, cos_ref, sin_ref, segc_ref, segr_ref, q_ref, g_ref, dq_ref, pair_ref, k_s, kt_s, v_s, bias_s, dk_s, dv_s):
    tok, hd = k_s.shape
    per_head = q_ref.shape[1] // hd
    tiles = tok // QT
    inv_root = hd ** -0.5
    scale = inv_root * 1.4426950408889634
    f32, bf16 = jnp.float32, jnp.bfloat16

    raw = proj_ref[:, :hd]
    keys = (raw * cos_ref[...] + pltpu.roll(raw, hd // 2, 1) * sin_ref[...]).astype(bf16)
    k_s[...] = keys
    kt_s[...] = keys.astype(f32).T.astype(bf16)
    v_s[...] = proj_ref[:, hd:].astype(bf16)
    dk_s[...] = jnp.zeros_like(dk_s)
    dv_s[...] = jnp.zeros_like(dv_s)
    for t in range(tiles):
        k0 = max(0, t - REACH) * QT
        k1 = (t + 1) * QT
        same = segc_ref[k0:k1, :] == segr_ref[0:1, t * QT:(t + 1) * QT]
        kpos = lax.broadcasted_iota(jnp.int32, (k1 - k0, QT), 0) + k0
        qpos = lax.broadcasted_iota(jnp.int32, (k1 - k0, QT), 1) + t * QT
        bias_s[t, 0:k1 - k0, :] = jnp.where(same & (kpos <= qpos), 0.0, NEG)

    def two_heads(hp, carry):
        c0 = pl.multiple_of(hp * 2 * hd, hd)
        c1 = pl.multiple_of(hp * 2 * hd + hd, hd)
        for t in range(tiles):
            k0 = max(0, t - REACH) * QT
            k1 = (t + 1) * QT
            rows = pl.ds(t * QT, QT)
            q2 = jnp.concatenate([q_ref[rows, pl.ds(c0, hd)], q_ref[rows, pl.ds(c1, hd)]], axis=0)
            g2 = jnp.concatenate([g_ref[rows, pl.ds(c0, hd)], g_ref[rows, pl.ds(c1, hd)]], axis=0)
            nt = (((1,), (1,)), ((), ()))
            bias = bias_s[t, 0:k1 - k0, :]
            bias = jnp.concatenate([bias, bias], axis=1)
            s = lax.dot_general(k_s[k0:k1, :], q2, nt, preferred_element_type=f32) * scale + bias
            e = jnp.exp2(s - jnp.max(s, axis=0, keepdims=True))
            p = e * (1.0 / jnp.sum(e, axis=0, keepdims=True))
            pb = p.astype(bf16)
            dp = lax.dot_general(v_s[k0:k1, :], g2, nt, preferred_element_type=f32)
            rd = jnp.sum(pb.astype(f32) * dp, axis=0, keepdims=True)
            ds = (p * (dp - rd)).astype(bf16)
            dv_s[k0:k1, :] += jnp.dot(pb, g2, preferred_element_type=f32)
            dk_s[k0:k1, :] += jnp.dot(ds, q2, preferred_element_type=f32)
            dqt = jnp.dot(kt_s[:, k0:k1], ds, preferred_element_type=f32) * inv_root
            dq_ref[rows, pl.ds(c0, hd)] = dqt[:, :QT].T.astype(bf16)
            dq_ref[rows, pl.ds(c1, hd)] = dqt[:, QT:].T.astype(bf16)
        return carry

    lax.fori_loop(0, per_head // 2, two_heads, 0)
    rot = dk_s[...] * inv_root
    pair_ref[:, :hd] = (rot * cos_ref[...] - pltpu.roll(rot, hd // 2, 1) * sin_ref[...]).astype(bf16)
    pair_ref[:, hd:] = dv_s[...].astype(bf16)


def attention(proj, cos, sin, segc, segr, q2d, g2d, hd, head0=0):
    tok = proj.shape[0]
    heads = proj.shape[1] // (2 * hd)
    total = q2d.shape[1] // hd
    return functools.partial(_attention, tok, heads, hd, head0)(proj, cos, sin, segc, segr, q2d, g2d)


def _attention(tok, heads, hd, head0, proj, cos, sin, segc, segr, q2d, g2d, per_head=8):
    wide = per_head * hd
    full = lambda a: pl.BlockSpec(a.shape, lambda i: (0, 0))
    col = lambda w, off=0: pl.BlockSpec((tok, w), lambda i: (0, i + off))
    tiles = tok // QT
    span = min(REACH + 1, tiles) * QT
    work = tok * span * heads * per_head
    return pl.pallas_call(
        attn_kernel,
        grid=(heads,),
        in_specs=[col(2 * hd), full(cos), full(sin), full(segc), full(segr), col(wide, head0), col(wide, head0)],
        out_specs=[col(wide), col(2 * hd)],
        out_shape=[
            jax.ShapeDtypeStruct((tok, heads * wide), jnp.bfloat16),
            jax.ShapeDtypeStruct((tok, heads * 2 * hd), jnp.bfloat16),
        ],
        scratch_shapes=[
            pltpu.VMEM((tok, hd), jnp.bfloat16),
            pltpu.VMEM((hd, tok), jnp.bfloat16),
            pltpu.VMEM((tok, hd), jnp.bfloat16),
            pltpu.VMEM((tiles, span, QT), jnp.float32),
            pltpu.VMEM((tok, hd), jnp.float32),
            pltpu.VMEM((tok, hd), jnp.float32),
        ],
        cost_estimate=pl.CostEstimate(flops=10 * work * hd, bytes_accessed=6 * tok * heads * wide, transcendentals=work),
        name="attn",
    )(proj, cos, sin, segc, segr, q2d, g2d)


def rope_tables(tok, hd):
    frequency = 500000.0 ** (-2.0 * jnp.arange(hd // 2, dtype=jnp.float32) / hd)
    angle = jnp.arange(tok, dtype=jnp.float32)[:, None] * frequency[None, :]
    cos, sin = jnp.cos(angle), jnp.sin(angle)
    return jnp.concatenate([cos, cos], axis=1), jnp.concatenate([-sin, sin], axis=1)


def seg_tables(seg_row):
    tok = seg_row.shape[0]
    return jnp.broadcast_to(seg_row[:, None], (tok, 128)), jnp.broadcast_to(seg_row[None, :], (8, tok))


def local(tokens, queries, out_grad, segment_ids, weight_slots, old_place, new_place):
    tok = tokens.shape[0]
    slot_rows, heads, _, hd = weight_slots.shape
    wide = heads * 2 * hd
    slot_total = lax.axis_size("dp") * (slot_rows // BR)
    blocks = old_place.shape[0]
    q2d = queries.reshape(tok, -1)
    g2d = out_grad.reshape(tok, -1)
    cos, sin = rope_tables(tok, hd)
    segc, segr = seg_tables(segment_ids[0])

    gathered = lax.all_gather(weight_slots.reshape(slot_rows, wide), "dp", axis=0, tiled=True)
    weights = jnp.take(gathered.reshape(slot_total, BR, wide), old_place, axis=0, mode="clip").reshape(blocks * BR, wide)
    proj = jnp.dot(tokens, weights, preferred_element_type=jnp.float32)
    dq, pair = attention(proj, cos, sin, segc, segr, q2d, g2d, hd)

    seq_part = lax.dot_general(tokens, pair, (((0,), (0,)), ((), ())), preferred_element_type=jnp.float32).astype(jnp.bfloat16)
    hit = new_place[None, :] == jnp.arange(slot_total, dtype=jnp.int32)[:, None]
    slot_block = jnp.max(jnp.where(hit, jnp.arange(blocks, dtype=jnp.int32)[None, :], -1), axis=1)
    spread = jnp.take(seq_part.reshape(blocks, BR, wide), jnp.maximum(slot_block, 0), axis=0, mode="clip")
    spread = jnp.where((slot_block >= 0)[:, None, None], spread, 0)
    weight_grad = lax.psum_scatter(spread.reshape(slot_total * BR, wide), "dp", scatter_dimension=0, tiled=True)

    part = lax.dot_general(pair, weights, (((1,), (1,)), ((), ())), preferred_element_type=jnp.float32).astype(jnp.bfloat16)
    input_grad = lax.psum_scatter(part, "mp", scatter_dimension=1, tiled=True)
    return (
        input_grad,
        dq.reshape(queries.shape),
        weight_grad.astype(jnp.float32).reshape(slot_rows, heads, 2, hd),
    )


def solution(mesh):
    return jax.shard_map(
        local,
        mesh=mesh,
        in_specs=(
            P("dp", None),
            P("dp", "mp", None),
            P("dp", "mp", None),
            P("dp", None),
            P("dp", "mp", None, None),
            P(),
            P(),
        ),
        out_specs=(P("dp", "mp"), P("dp", "mp", None), P("dp", "mp", None, None)),
        check_vma=False,
    )
```

```python
import functools

import jax
import jax.numpy as jnp
from jax import lax
from jax.experimental import pallas as pl
from jax.experimental.pallas import tpu as pltpu
from jax.sharding import PartitionSpec as P


BR = 128
QT = 128
REACH = 2
NEG = -1e30


def attn_kernel(proj_ref, cos_ref, sin_ref, segc_ref, segr_ref, q_ref, g_ref, dq_ref, pair_ref, k_s, kt_s, v_s, bias_s, dk_s, dv_s):
    tok, hd = k_s.shape
    per_head = q_ref.shape[1] // hd
    tiles = tok // QT
    inv_root = hd ** -0.5
    scale = inv_root * 1.4426950408889634
    f32, bf16 = jnp.float32, jnp.bfloat16

    raw = proj_ref[:, :hd]
    keys = (raw * cos_ref[...] + pltpu.roll(raw, hd // 2, 1) * sin_ref[...]).astype(bf16)
    k_s[...] = keys
    kt_s[...] = keys.astype(f32).T.astype(bf16)
    v_s[...] = proj_ref[:, hd:].astype(bf16)
    dk_s[...] = jnp.zeros_like(dk_s)
    dv_s[...] = jnp.zeros_like(dv_s)
    for t in range(tiles):
        k0 = max(0, t - REACH) * QT
        k1 = (t + 1) * QT
        same = segc_ref[k0:k1, :] == segr_ref[0:1, t * QT:(t + 1) * QT]
        kpos = lax.broadcasted_iota(jnp.int32, (k1 - k0, QT), 0) + k0
        qpos = lax.broadcasted_iota(jnp.int32, (k1 - k0, QT), 1) + t * QT
        bias_s[t, 0:k1 - k0, :] = jnp.where(same & (kpos <= qpos), 0.0, NEG)

    def two_heads(hp, carry):
        c0 = pl.multiple_of(hp * 2 * hd, hd)
        c1 = pl.multiple_of(hp * 2 * hd + hd, hd)
        for t in range(tiles):
            k0 = max(0, t - REACH) * QT
            k1 = (t + 1) * QT
            rows = pl.ds(t * QT, QT)
            q2 = jnp.concatenate([q_ref[rows, pl.ds(c0, hd)], q_ref[rows, pl.ds(c1, hd)]], axis=0)
            g2 = jnp.concatenate([g_ref[rows, pl.ds(c0, hd)], g_ref[rows, pl.ds(c1, hd)]], axis=0)
            nt = (((1,), (1,)), ((), ()))
            bias = bias_s[t, 0:k1 - k0, :]
            bias = jnp.concatenate([bias, bias], axis=1)
            s = lax.dot_general(k_s[k0:k1, :], q2, nt, preferred_element_type=f32) * scale + bias
            e = jnp.exp2(s - jnp.max(s, axis=0, keepdims=True))
            p = e * (1.0 / jnp.sum(e, axis=0, keepdims=True))
            pb = p.astype(bf16)
            dp = lax.dot_general(v_s[k0:k1, :], g2, nt, preferred_element_type=f32)
            rd = jnp.sum(pb.astype(f32) * dp, axis=0, keepdims=True)
            ds = (p * (dp - rd)).astype(bf16)
            dv_s[k0:k1, :] += jnp.dot(pb, g2, preferred_element_type=f32)
            dk_s[k0:k1, :] += jnp.dot(ds, q2, preferred_element_type=f32)
            dqt = jnp.dot(kt_s[:, k0:k1], ds, preferred_element_type=f32) * inv_root
            dq_ref[rows, pl.ds(c0, hd)] = dqt[:, :QT].T.astype(bf16)
            dq_ref[rows, pl.ds(c1, hd)] = dqt[:, QT:].T.astype(bf16)
        return carry

    lax.fori_loop(0, per_head // 2, two_heads, 0)
    rot = dk_s[...] * inv_root
    pair_ref[:, :hd] = (rot * cos_ref[...] - pltpu.roll(rot, hd // 2, 1) * sin_ref[...]).astype(bf16)
    pair_ref[:, hd:] = dv_s[...].astype(bf16)


def attention(proj, cos, sin, segc, segr, q2d, g2d, hd, head0=0):
    tok = proj.shape[0]
    heads = proj.shape[1] // (2 * hd)
    return functools.partial(_attention, tok, heads, hd, head0)(proj, cos, sin, segc, segr, q2d, g2d)


def _attention(tok, heads, hd, head0, proj, cos, sin, segc, segr, q2d, g2d, per_head=8):
    wide = per_head * hd
    full = lambda a: pl.BlockSpec(a.shape, lambda i: (0, 0))
    col = lambda w, off=0: pl.BlockSpec((tok, w), lambda i: (0, i + off))
    tiles = tok // QT
    span = min(REACH + 1, tiles) * QT
    work = tok * span * heads * per_head
    return pl.pallas_call(
        attn_kernel,
        grid=(heads,),
        in_specs=[col(2 * hd), full(cos), full(sin), full(segc), full(segr), col(wide, head0), col(wide, head0)],
        out_specs=[col(wide), col(2 * hd)],
        out_shape=[
            jax.ShapeDtypeStruct((tok, heads * wide), jnp.bfloat16),
            jax.ShapeDtypeStruct((tok, heads * 2 * hd), jnp.bfloat16),
        ],
        scratch_shapes=[
            pltpu.VMEM((tok, hd), jnp.bfloat16),
            pltpu.VMEM((hd, tok), jnp.bfloat16),
            pltpu.VMEM((tok, hd), jnp.bfloat16),
            pltpu.VMEM((tiles, span, QT), jnp.float32),
            pltpu.VMEM((tok, hd), jnp.float32),
            pltpu.VMEM((tok, hd), jnp.float32),
        ],
        cost_estimate=pl.CostEstimate(flops=10 * work * hd, bytes_accessed=6 * tok * heads * wide, transcendentals=work),
        name="attn",
    )(proj, cos, sin, segc, segr, q2d, g2d)


def rope_tables(tok, hd):
    frequency = 500000.0 ** (-2.0 * jnp.arange(hd // 2, dtype=jnp.float32) / hd)
    angle = jnp.arange(tok, dtype=jnp.float32)[:, None] * frequency[None, :]
    cos, sin = jnp.cos(angle), jnp.sin(angle)
    return jnp.concatenate([cos, cos], axis=1), jnp.concatenate([-sin, sin], axis=1)


def seg_tables(seg_row):
    tok = seg_row.shape[0]
    return jnp.broadcast_to(seg_row[:, None], (tok, 128)), jnp.broadcast_to(seg_row[None, :], (8, tok))


def ring_order(chips):
    rows = 1
    while rows * rows < chips:
        rows *= 2
    cols = chips // rows
    if cols == 1:
        return list(range(chips))
    walk = [(0, 0)]
    for x in range(cols):
        zs = range(1, rows) if x % 2 == 0 else range(rows - 1, 0, -1)
        walk += [(z, x) for z in zs]
    walk += [(0, x) for x in range(cols - 1, 0, -1)]
    return [z * cols + x for z, x in walk]


class Ring:
    def __init__(self, dp, slots, blocks):
        self.dp, self.slots, self.blocks = dp, slots, blocks
        self.chips = dp // 2
        self.order = ring_order(self.chips)
        self.win = max(1, blocks // self.chips // 2)
        self.steps = -(-(blocks - self.win) // (2 * self.win))
        self.depth = self.win * self.steps
        self.cap = 2 * slots
        self.core_swap = [(d, d ^ 1) for d in range(dp)]
        n = self.chips
        up = [(self.order[k], self.order[(k + 1) % n]) for k in range(n)]
        self.gather_hop = [(2 * a, 2 * b) for a, b in up] + [(2 * b + 1, 2 * a + 1) for a, b in up]
        self.reduce_hop = [(b, a) for a, b in self.gather_hop]

    def plan(self, place):
        i32 = jnp.int32
        ks = jnp.arange(self.chips, dtype=i32)
        order = jnp.array(self.order, dtype=i32)
        blk = jnp.arange(self.blocks, dtype=i32)
        chip = place // self.cap
        at_chip = chip[:, None] == order[None, :]
        rho = jnp.sum(jnp.where(at_chip, ks[None, :], 0), axis=1)
        count = jnp.sum(at_chip.astype(i32), axis=0)
        virt = jnp.maximum(count, self.win)
        start = jnp.sum(jnp.where(ks[None, :] < ks[:, None], virt[None, :], 0), axis=1)
        total = jnp.sum(virt)
        inside = jnp.sum(((chip[:, None] == chip[None, :]) & (place[None, :] < place[:, None])).astype(i32), axis=1)
        vrank = jnp.sum(jnp.where(at_chip, start[None, :], 0), axis=1) + inside
        dev = lax.axis_index("dp").astype(i32)
        mine = order == dev // 2
        s0 = jnp.sum(jnp.where(mine, start, 0))
        nv = jnp.sum(jnp.where(mine, virt, 0))
        core = dev % 2
        ok = total <= 2 * self.depth + self.win

        def ranks(kind, pos):
            rank = jnp.where(kind == 0, s0 + nv - 1 - pos, s0 + pos)
            return rank + jnp.where(rank < 0, total, 0) - jnp.where(rank >= total, total, 0)

        def lookup(rank):
            return jnp.max(jnp.where(vrank[None, :] == rank[:, None], blk[None, :], -1), axis=1)

        def reach(kind):
            return (total - nv + 1 - kind) // 2

        d = jnp.arange(self.depth, dtype=i32)

        def window_table(kind):
            return jnp.where(d < reach(kind), lookup(ranks(kind, nv + d)), -1)

        q = jnp.arange(self.slots, dtype=i32)

        def hits(device):
            return place[None, :] == (device * self.slots + q)[:, None]

        def own_table(device):
            return jnp.max(jnp.where(hits(device), blk[None, :], -1), axis=1)

        def slot_table(device):
            hit = hits(device)
            local_at = jnp.sum(jnp.where(hit, inside[None, :], 0), axis=1)
            pos = jnp.where(core == 0, nv - 1 - local_at, local_at)
            return jnp.where(jnp.any(hit, axis=1), self.cap - nv + pos, -1)

        return dict(
            ok=ok, nv=nv,
            here=jnp.concatenate([own_table(dev), window_table(core)]),
            there=jnp.concatenate([own_table(dev ^ 1), window_table(1 - core)]),
            own=slot_table(dev), other=slot_table(dev ^ 1),
        )


def take_blocks(table, src):
    got = jnp.take(src.reshape(-1, BR, src.shape[1]), jnp.maximum(table, 0), axis=0, mode="clip")
    return jnp.where((table >= 0)[:, None, None], got, 0).reshape(-1, src.shape[1])


def masked(ref, flag):
    return jnp.where(flag, ref[...], jnp.zeros_like(ref))


def pick_blocks(table, src):
    count, w = table.shape[0], src.shape[1]
    per = 4 if count % 4 == 0 else 1

    def kernel(tbl, *refs):
        for j in range(per):
            live = tbl[pl.program_id(0) * per + j] >= 0
            refs[per][j * BR:(j + 1) * BR, :] = masked(refs[j], live)

    block = lambda j: pl.BlockSpec((BR, w), lambda i, tbl: (jnp.maximum(tbl[i * per + j], 0), 0))
    return pl.pallas_call(
        kernel,
        grid_spec=pltpu.PrefetchScalarGridSpec(
            num_scalar_prefetch=1, grid=(count // per,),
            in_specs=[block(j) for j in range(per)],
            out_specs=pl.BlockSpec((per * BR, w), lambda i, tbl: (i, 0)),
        ),
        out_shape=jax.ShapeDtypeStruct((count * BR, w), src.dtype),
        name="pick",
    )(table, *[src] * per)


def emit_blocks(table, base, came, far):
    n = len(came)
    wide = base.shape[1]
    w = wide // n
    parts = wide // 128

    def kernel(tbl, base_ref, *rest):
        out_ref = rest[-1]
        live = tbl[pl.program_id(0)] >= 0
        for k in range(n):
            cols = slice(k * w, (k + 1) * w)
            total = base_ref[:, cols].astype(jnp.float32) + rest[n + k][...].astype(jnp.float32)
            total = total + masked(rest[k], live).astype(jnp.float32)
            for j in range(w // 128):
                out_ref[pl.ds(k * (w // 128) + j, BR, stride=parts), :] = total[:, j * 128:(j + 1) * 128]

    here = lambda width: pl.BlockSpec((BR, width), lambda i, tbl: (i, 0))
    picked = pl.BlockSpec((BR, w), lambda i, tbl: (jnp.maximum(tbl[i], 0), 0))
    rows = table.shape[0] * BR
    return pl.pallas_call(
        kernel,
        grid_spec=pltpu.PrefetchScalarGridSpec(
            num_scalar_prefetch=1, grid=table.shape,
            in_specs=[here(wide)] + [picked] * n + [here(w)] * n,
            out_specs=pl.BlockSpec((BR * parts, 128), lambda i, tbl: (i, 0)),
        ),
        out_shape=jax.ShapeDtypeStruct((rows * parts, 128), jnp.float32),
        name="emit",
    )(table, base, *came, *far)


def project(table, tokens, slots3):
    tok, feats = tokens.shape
    wide = slots3.shape[2]
    per = 4

    def kernel(tbl, tok_ref, *rest):
        out_ref = rest[-1]

        @pl.when(pl.program_id(0) == 0)
        def _():
            out_ref[...] = jnp.zeros_like(out_ref)

        w = jnp.concatenate([r[0] for r in rest[:per]], axis=0)
        out_ref[...] += jnp.dot(tok_ref[...], w, preferred_element_type=jnp.float32)

    block = lambda j: pl.BlockSpec((1, BR, wide), lambda i, tbl: (tbl[i * per + j], 0, 0))
    return pl.pallas_call(
        kernel,
        grid_spec=pltpu.PrefetchScalarGridSpec(
            num_scalar_prefetch=1, grid=(feats // (per * BR),),
            in_specs=[pl.BlockSpec((tok, per * BR), lambda i, tbl: (0, i))] + [block(j) for j in range(per)],
            out_specs=pl.BlockSpec((tok, wide), lambda i, tbl: (0, 0)),
        ),
        out_shape=jax.ShapeDtypeStruct((tok, wide), jnp.float32),
        cost_estimate=pl.CostEstimate(flops=2 * tok * feats * wide, bytes_accessed=2 * feats * (wide + tok), transcendentals=0),
        name="project",
    )(table, tokens, *[slots3] * per)


def unproject(table, pair, slots3, extra=None):
    tok, wide = pair.shape
    per = 4
    cols = table.shape[0] * BR
    nt = (((1,), (1,)), ((), ()))
    more = () if extra is None else (extra,)

    def kernel(tbl, pair_ref, *rest):
        out_ref = rest[-1]
        w = jnp.concatenate([r[0] for r in rest[:per]], axis=0)
        total = lax.dot_general(pair_ref[...], w, nt, preferred_element_type=jnp.float32)
        if more:
            total = total + rest[per][...].astype(jnp.float32)
        out_ref[...] = total.astype(out_ref.dtype)

    block = lambda j: pl.BlockSpec((1, BR, wide), lambda i, tbl: (tbl[i * per + j], 0, 0))
    tile = pl.BlockSpec((tok, per * BR), lambda i, tbl: (0, i))
    return pl.pallas_call(
        kernel,
        grid_spec=pltpu.PrefetchScalarGridSpec(
            num_scalar_prefetch=1, grid=(cols // (per * BR),),
            in_specs=[pl.BlockSpec((tok, wide), lambda i, tbl: (0, 0))] + [block(j) for j in range(per)] + [tile] * len(more),
            out_specs=tile,
        ),
        out_shape=jax.ShapeDtypeStruct((tok, cols), jnp.bfloat16),
        cost_estimate=pl.CostEstimate(flops=2 * tok * cols * wide, bytes_accessed=2 * cols * (wide + tok), transcendentals=0),
        name="unproject",
    )(table, pair, *[slots3] * per, *more)


def ring_reduce(ring, plan, tok_pair, pair, pair_both, side, finish):
    f32, bf16 = jnp.float32, jnp.bfloat16
    width = pair_both.shape[1]
    streams = 2 if width % 512 == 0 else 1
    w = width // streams
    wr = ring.win * BR
    base = ring.slots * BR
    got = [jnp.zeros(((ring.cap + ring.depth) * BR, w), bf16) for _ in range(streams)]
    near = ring.cap * BR
    group = 2 if ring.steps % 2 == 0 else 1
    rhs = [pair_both[:, i * w:(i + 1) * w] for i in range(streams)]
    chunk = [None] * streams
    aside = None
    for s in range(ring.steps - 1, -1, -1):
        first = s == ring.steps - 1
        at = (s % group) * wr
        for i in range(streams):
            if (s + 1) % group == 0:
                lo = base + (s + 1 - group) * wr
                chunk[i] = jnp.dot(tok_pair[lo:lo + group * wr], rhs[i], preferred_element_type=f32).astype(bf16)
            sent = chunk[i][at:at + wr]
            if not first:
                here = got[i][near + s * wr:near + (s + 1) * wr]
                sent = (sent.astype(f32) + here.astype(f32)).astype(bf16)
            moved = lax.ppermute(sent, "dp", ring.reduce_hop)
            if first and i == 0:
                ready, moved = lax.optimization_barrier((pair, moved))
                aside = side(ready)
            got[i] = lax.dynamic_update_slice(got[i], moved, ((ring.cap - plan["nv"] + ring.win * s) * BR, 0))
            if (s % group) == 0 and s > 0:
                extra = [aside] if s == ring.steps - group and i == 0 else []
                tied = lax.optimization_barrier((rhs[i], moved, *extra))
                rhs[i] = tied[0]
                if extra:
                    aside = finish(tied[2])
    own = jnp.concatenate([jnp.dot(tok_pair[:base], r, preferred_element_type=f32).astype(bf16) for r in rhs], axis=1)
    far = [lax.ppermute(pick_blocks(plan["other"], g), "dp", ring.core_swap) for g in got]
    return emit_blocks(plan["own"], own, got, far), aside


def local(tokens, queries, out_grad, segment_ids, weight_slots, old_place, new_place):
    tok, _ = tokens.shape
    slot_rows, heads, _, hd = weight_slots.shape
    wide = heads * 2 * hd
    dp, mp = lax.axis_size("dp"), lax.axis_size("mp")
    slots = slot_rows // BR
    slot_total = dp * slots
    blocks = old_place.shape[0]
    f32, bf16 = jnp.float32, jnp.bfloat16
    q2d = queries.reshape(tok, -1)
    g2d = out_grad.reshape(tok, -1)
    cos, sin = rope_tables(tok, hd)
    segc, segr = seg_tables(segment_ids[0])

    gathered = lax.all_gather(weight_slots.reshape(slot_rows, wide), "dp", axis=0, tiled=True)

    ring = Ring(dp, slots, blocks)
    plan = ring.plan(new_place)
    tok_t = tokens.T
    tok_here = take_blocks(plan["here"], tok_t)
    tok_there = lax.ppermute(take_blocks(plan["there"], tok_t), "dp", ring.core_swap)
    tok_pair = jnp.concatenate([tok_here, tok_there], axis=1)

    slots3 = gathered.reshape(slot_total, BR, wide)
    proj = project(old_place, tokens, slots3)
    dq, pair = attention(proj, cos, sin, segc, segr, q2d, g2d, hd)

    def feature_part(pair):
        if mp == 2:
            half = blocks // 2
            away = lax.dynamic_slice(old_place, ((1 - lax.axis_index("mp")) * half,), (half,))
            return unproject(away, pair, slots3)
        return unproject(old_place, pair, slots3)

    def feature_carry(part):
        if mp == 2:
            return lax.ppermute(part, "mp", [(0, 1), (1, 0)])
        return lax.psum_scatter(part, "mp", scatter_dimension=1, tiled=True)

    def feature_end(pair, got):
        if mp == 2:
            half = blocks // 2
            home = lax.dynamic_slice(old_place, (lax.axis_index("mp") * half,), (half,))
            return unproject(home, pair, slots3, got)
        return got

    def fast(tok_pair, tokens, pair, dq, slots3):
        far = lax.ppermute(pair, "dp", ring.core_swap)
        both = jnp.concatenate([pair, far], axis=0)
        wg, got = ring_reduce(ring, plan, tok_pair, pair, both, feature_part, feature_carry)
        return feature_end(pair, got), dq.reshape(queries.shape), wg.reshape(slot_rows, heads, 2, hd)

    def slow(tok_pair, tokens, pair, dq, slots3):
        part = lax.dot_general(tokens, pair, (((0,), (0,)), ((), ())), preferred_element_type=f32).astype(bf16)
        hit = new_place[None, :] == jnp.arange(slot_total, dtype=jnp.int32)[:, None]
        slot_block = jnp.max(jnp.where(hit, jnp.arange(blocks, dtype=jnp.int32)[None, :], -1), axis=1)
        wg = lax.psum_scatter(take_blocks(slot_block, part), "dp", scatter_dimension=0, tiled=True).astype(f32)
        return feature_end(pair, feature_carry(feature_part(pair))), dq.reshape(queries.shape), wg.reshape(slot_rows, heads, 2, hd)

    return lax.cond(plan["ok"], fast, slow, tok_pair, tokens, pair, dq, slots3)


def solution(mesh):
    return jax.shard_map(
        local,
        mesh=mesh,
        in_specs=(
            P("dp", None),
            P("dp", "mp", None),
            P("dp", "mp", None),
            P("dp", None),
            P("dp", "mp", None, None),
            P(),
            P(),
        ),
        out_specs=(P("dp", "mp"), P("dp", "mp", None), P("dp", "mp", None, None)),
        check_vma=False,
    )
```

```python
import functools

import jax
import jax.numpy as jnp
from jax import lax
from jax.experimental import pallas as pl
from jax.experimental.pallas import tpu as pltpu
from jax.sharding import PartitionSpec as P


BR = 128
QT = 128
REACH = 2
NEG = -1e30


def attn_kernel(proj_ref, cos_ref, sin_ref, segc_ref, segr_ref, q_ref, g_ref, dq_ref, pair_ref, k_s, kt_s, v_s, bias_s, dk_s, dv_s):
    tok, hd = k_s.shape
    per_head = q_ref.shape[1] // hd
    tiles = tok // QT
    inv_root = hd ** -0.5
    scale = inv_root * 1.4426950408889634
    f32, bf16 = jnp.float32, jnp.bfloat16

    raw = proj_ref[:, :hd]
    keys = (raw * cos_ref[...] + pltpu.roll(raw, hd // 2, 1) * sin_ref[...]).astype(bf16)
    k_s[...] = keys
    kt_s[...] = keys.astype(f32).T.astype(bf16)
    v_s[...] = proj_ref[:, hd:].astype(bf16)
    dk_s[...] = jnp.zeros_like(dk_s)
    dv_s[...] = jnp.zeros_like(dv_s)
    for t in range(tiles):
        k0 = max(0, t - REACH) * QT
        k1 = (t + 1) * QT
        same = segc_ref[k0:k1, :] == segr_ref[0:1, t * QT:(t + 1) * QT]
        kpos = lax.broadcasted_iota(jnp.int32, (k1 - k0, QT), 0) + k0
        qpos = lax.broadcasted_iota(jnp.int32, (k1 - k0, QT), 1) + t * QT
        bias_s[t, 0:k1 - k0, :] = jnp.where(same & (kpos <= qpos), 0.0, NEG)

    def two_heads(hp, carry):
        c0 = pl.multiple_of(hp * 2 * hd, hd)
        c1 = pl.multiple_of(hp * 2 * hd + hd, hd)
        for t in range(tiles):
            k0 = max(0, t - REACH) * QT
            k1 = (t + 1) * QT
            rows = pl.ds(t * QT, QT)
            q2 = jnp.concatenate([q_ref[rows, pl.ds(c0, hd)], q_ref[rows, pl.ds(c1, hd)]], axis=0)
            g2 = jnp.concatenate([g_ref[rows, pl.ds(c0, hd)], g_ref[rows, pl.ds(c1, hd)]], axis=0)
            nt = (((1,), (1,)), ((), ()))
            bias = bias_s[t, 0:k1 - k0, :]
            bias = jnp.concatenate([bias, bias], axis=1)
            s = lax.dot_general(k_s[k0:k1, :], q2, nt, preferred_element_type=f32) * scale + bias
            e = jnp.exp2(s - jnp.max(s, axis=0, keepdims=True))
            p = e * (1.0 / jnp.sum(e, axis=0, keepdims=True))
            pb = p.astype(bf16)
            dp = lax.dot_general(v_s[k0:k1, :], g2, nt, preferred_element_type=f32)
            rd = jnp.sum(pb.astype(f32) * dp, axis=0, keepdims=True)
            ds = (p * (dp - rd)).astype(bf16)
            dv_s[k0:k1, :] += jnp.dot(pb, g2, preferred_element_type=f32)
            dk_s[k0:k1, :] += jnp.dot(ds, q2, preferred_element_type=f32)
            dqt = jnp.dot(kt_s[:, k0:k1], ds, preferred_element_type=f32) * inv_root
            dq_ref[rows, pl.ds(c0, hd)] = dqt[:, :QT].T.astype(bf16)
            dq_ref[rows, pl.ds(c1, hd)] = dqt[:, QT:].T.astype(bf16)
        return carry

    lax.fori_loop(0, per_head // 2, two_heads, 0)
    rot = dk_s[...] * inv_root
    pair_ref[:, :hd] = (rot * cos_ref[...] - pltpu.roll(rot, hd // 2, 1) * sin_ref[...]).astype(bf16)
    pair_ref[:, hd:] = dv_s[...].astype(bf16)


def attention(proj, cos, sin, segc, segr, q2d, g2d, hd, head0=0):
    tok = proj.shape[0]
    heads = proj.shape[1] // (2 * hd)
    return functools.partial(_attention, tok, heads, hd, head0)(proj, cos, sin, segc, segr, q2d, g2d)


def _attention(tok, heads, hd, head0, proj, cos, sin, segc, segr, q2d, g2d, per_head=8):
    wide = per_head * hd
    full = lambda a: pl.BlockSpec(a.shape, lambda i: (0, 0))
    col = lambda w, off=0: pl.BlockSpec((tok, w), lambda i: (0, i + off))
    tiles = tok // QT
    span = min(REACH + 1, tiles) * QT
    work = tok * span * heads * per_head
    return pl.pallas_call(
        attn_kernel,
        grid=(heads,),
        in_specs=[col(2 * hd), full(cos), full(sin), full(segc), full(segr), col(wide, head0), col(wide, head0)],
        out_specs=[col(wide), col(2 * hd)],
        out_shape=[
            jax.ShapeDtypeStruct((tok, heads * wide), jnp.bfloat16),
            jax.ShapeDtypeStruct((tok, heads * 2 * hd), jnp.bfloat16),
        ],
        scratch_shapes=[
            pltpu.VMEM((tok, hd), jnp.bfloat16),
            pltpu.VMEM((hd, tok), jnp.bfloat16),
            pltpu.VMEM((tok, hd), jnp.bfloat16),
            pltpu.VMEM((tiles, span, QT), jnp.float32),
            pltpu.VMEM((tok, hd), jnp.float32),
            pltpu.VMEM((tok, hd), jnp.float32),
        ],
        cost_estimate=pl.CostEstimate(flops=10 * work * hd, bytes_accessed=6 * tok * heads * wide, transcendentals=work),
        name="attn",
    )(proj, cos, sin, segc, segr, q2d, g2d)


def rope_tables(tok, hd):
    frequency = 500000.0 ** (-2.0 * jnp.arange(hd // 2, dtype=jnp.float32) / hd)
    angle = jnp.arange(tok, dtype=jnp.float32)[:, None] * frequency[None, :]
    cos, sin = jnp.cos(angle), jnp.sin(angle)
    return jnp.concatenate([cos, cos], axis=1), jnp.concatenate([-sin, sin], axis=1)


def seg_tables(seg_row):
    tok = seg_row.shape[0]
    return jnp.broadcast_to(seg_row[:, None], (tok, 128)), jnp.broadcast_to(seg_row[None, :], (8, tok))


def ring_order(chips):
    rows = 1
    while rows * rows < chips:
        rows *= 2
    cols = chips // rows
    if cols == 1:
        return list(range(chips))
    walk = [(0, 0)]
    for x in range(cols):
        zs = range(1, rows) if x % 2 == 0 else range(rows - 1, 0, -1)
        walk += [(z, x) for z in zs]
    walk += [(0, x) for x in range(cols - 1, 0, -1)]
    return [z * cols + x for z, x in walk]


class Ring:
    def __init__(self, dp, slots, blocks):
        self.dp, self.slots, self.blocks = dp, slots, blocks
        self.chips = dp // 2
        self.order = ring_order(self.chips)
        self.win = max(1, blocks // self.chips // 2)
        self.steps = -(-(blocks - self.win) // (2 * self.win))
        self.depth = self.win * self.steps
        self.cap = 2 * slots
        self.core_swap = [(d, d ^ 1) for d in range(dp)]
        n = self.chips
        up = [(self.order[k], self.order[(k + 1) % n]) for k in range(n)]
        self.gather_hop = [(2 * a, 2 * b) for a, b in up] + [(2 * b + 1, 2 * a + 1) for a, b in up]
        self.reduce_hop = [(b, a) for a, b in self.gather_hop]

    def plan(self, place):
        i32 = jnp.int32
        ks = jnp.arange(self.chips, dtype=i32)
        order = jnp.array(self.order, dtype=i32)
        blk = jnp.arange(self.blocks, dtype=i32)
        chip = place // self.cap
        at_chip = chip[:, None] == order[None, :]
        rho = jnp.sum(jnp.where(at_chip, ks[None, :], 0), axis=1)
        count = jnp.sum(at_chip.astype(i32), axis=0)
        virt = jnp.maximum(count, self.win)
        start = jnp.sum(jnp.where(ks[None, :] < ks[:, None], virt[None, :], 0), axis=1)
        total = jnp.sum(virt)
        inside = jnp.sum(((chip[:, None] == chip[None, :]) & (place[None, :] < place[:, None])).astype(i32), axis=1)
        vrank = jnp.sum(jnp.where(at_chip, start[None, :], 0), axis=1) + inside
        dev = lax.axis_index("dp").astype(i32)
        mine = order == dev // 2
        s0 = jnp.sum(jnp.where(mine, start, 0))
        nv = jnp.sum(jnp.where(mine, virt, 0))
        core = dev % 2
        ok = total <= 2 * self.depth + self.win

        def ranks(kind, pos):
            rank = jnp.where(kind == 0, s0 + nv - 1 - pos, s0 + pos)
            return rank + jnp.where(rank < 0, total, 0) - jnp.where(rank >= total, total, 0)

        def lookup(rank):
            return jnp.max(jnp.where(vrank[None, :] == rank[:, None], blk[None, :], -1), axis=1)

        def reach(kind):
            return (total - nv + 1 - kind) // 2

        d = jnp.arange(self.depth, dtype=i32)

        def window_table(kind):
            return jnp.where(d < reach(kind), lookup(ranks(kind, nv + d)), -1)

        q = jnp.arange(self.slots, dtype=i32)

        def hits(device):
            return place[None, :] == (device * self.slots + q)[:, None]

        def own_table(device):
            return jnp.max(jnp.where(hits(device), blk[None, :], -1), axis=1)

        def slot_table(device):
            hit = hits(device)
            local_at = jnp.sum(jnp.where(hit, inside[None, :], 0), axis=1)
            pos = jnp.where(core == 0, nv - 1 - local_at, local_at)
            return jnp.where(jnp.any(hit, axis=1), self.cap - nv + pos, -1)

        return dict(
            ok=ok, nv=nv,
            here=jnp.concatenate([own_table(dev), window_table(core)]),
            there=jnp.concatenate([own_table(dev ^ 1), window_table(1 - core)]),
            own=slot_table(dev), other=slot_table(dev ^ 1),
        )


def masked(ref, flag):
    return jnp.where(flag, ref[...], jnp.zeros_like(ref))


def pick_blocks(table, src):
    count, w = table.shape[0], src.shape[1]
    per = 4 if count % 4 == 0 else 1

    def kernel(tbl, *refs):
        for j in range(per):
            live = tbl[pl.program_id(0) * per + j] >= 0
            refs[per][j * BR:(j + 1) * BR, :] = masked(refs[j], live)

    block = lambda j: pl.BlockSpec((BR, w), lambda i, tbl: (jnp.maximum(tbl[i * per + j], 0), 0))
    return pl.pallas_call(
        kernel,
        grid_spec=pltpu.PrefetchScalarGridSpec(
            num_scalar_prefetch=1, grid=(count // per,),
            in_specs=[block(j) for j in range(per)],
            out_specs=pl.BlockSpec((per * BR, w), lambda i, tbl: (i, 0)),
        ),
        out_shape=jax.ShapeDtypeStruct((count * BR, w), src.dtype),
        name="pick",
    )(table, *[src] * per)


def emit_blocks(table, lhs, rhs, came, far):
    n = len(came)
    w = rhs[0].shape[1]
    parts = n * w // 128
    deep = lhs.shape[1]

    count = table.shape[0]
    per = 4 if count % 4 == 0 else 1
    rows = per * BR

    def kernel(tbl, lhs_ref, *rest):
        rhs_refs, far_refs, came_refs, out_ref = rest[:n], rest[n:2 * n], rest[2 * n:-1], rest[-1]
        for k in range(n):
            total = jnp.dot(lhs_ref[...], rhs_refs[k][...], preferred_element_type=jnp.float32)
            total = total + far_refs[k][...].astype(jnp.float32)
            for r in range(per):
                live = tbl[pl.program_id(0) * per + r] >= 0
                here = total[r * BR:(r + 1) * BR] + masked(came_refs[k * per + r], live).astype(jnp.float32)
                for j in range(w // 128):
                    first = r * BR * parts + k * (w // 128) + j
                    out_ref[pl.ds(first, BR, stride=parts), :] = here[:, j * 128:(j + 1) * 128]

    here = lambda width: pl.BlockSpec((rows, width), lambda i, tbl: (i, 0))
    whole = pl.BlockSpec((deep, w), lambda i, tbl: (0, 0))
    picked = [pl.BlockSpec((BR, w), lambda i, tbl, r=r: (jnp.maximum(tbl[i * per + r], 0), 0)) for r in range(per)]
    return pl.pallas_call(
        kernel,
        grid_spec=pltpu.PrefetchScalarGridSpec(
            num_scalar_prefetch=1, grid=(count // per,),
            in_specs=[here(deep)] + [whole] * n + [here(w)] * n + picked * n,
            out_specs=pl.BlockSpec((rows * parts, 128), lambda i, tbl: (i, 0)),
        ),
        out_shape=jax.ShapeDtypeStruct((count * BR * parts, 128), jnp.float32),
        name="emit",
    )(table, lhs, *rhs, *far, *[c for c in came for _ in range(per)])


def project(table, tokens, slots3):
    tok, feats = tokens.shape
    wide = slots3.shape[2]
    per = 4

    def kernel(tbl, tok_ref, *rest):
        out_ref = rest[-1]

        @pl.when(pl.program_id(0) == 0)
        def _():
            out_ref[...] = jnp.zeros_like(out_ref)

        w = jnp.concatenate([r[0] for r in rest[:per]], axis=0)
        out_ref[...] += jnp.dot(tok_ref[...], w, preferred_element_type=jnp.float32)

    block = lambda j: pl.BlockSpec((1, BR, wide), lambda i, tbl: (tbl[i * per + j], 0, 0))
    return pl.pallas_call(
        kernel,
        grid_spec=pltpu.PrefetchScalarGridSpec(
            num_scalar_prefetch=1, grid=(feats // (per * BR),),
            in_specs=[pl.BlockSpec((tok, per * BR), lambda i, tbl: (0, i))] + [block(j) for j in range(per)],
            out_specs=pl.BlockSpec((tok, wide), lambda i, tbl: (0, 0)),
        ),
        out_shape=jax.ShapeDtypeStruct((tok, wide), jnp.float32),
        cost_estimate=pl.CostEstimate(flops=2 * tok * feats * wide, bytes_accessed=2 * feats * (wide + tok), transcendentals=0),
        name="project",
    )(table, tokens, *[slots3] * per)


def unproject(table, pair, slots3, extra=None):
    tok, wide = pair.shape
    per = 4
    cols = table.shape[0] * BR
    nt = (((1,), (1,)), ((), ()))
    more = () if extra is None else (extra,)

    def kernel(tbl, pair_ref, *rest):
        out_ref = rest[-1]
        w = jnp.concatenate([r[0] for r in rest[:per]], axis=0)
        total = lax.dot_general(pair_ref[...], w, nt, preferred_element_type=jnp.float32)
        if more:
            total = total + rest[per][...].astype(jnp.float32)
        out_ref[...] = total.astype(out_ref.dtype)

    block = lambda j: pl.BlockSpec((1, BR, wide), lambda i, tbl: (tbl[i * per + j], 0, 0))
    tile = pl.BlockSpec((tok, per * BR), lambda i, tbl: (0, i))
    return pl.pallas_call(
        kernel,
        grid_spec=pltpu.PrefetchScalarGridSpec(
            num_scalar_prefetch=1, grid=(cols // (per * BR),),
            in_specs=[pl.BlockSpec((tok, wide), lambda i, tbl: (0, 0))] + [block(j) for j in range(per)] + [tile] * len(more),
            out_specs=tile,
        ),
        out_shape=jax.ShapeDtypeStruct((tok, cols), jnp.bfloat16),
        cost_estimate=pl.CostEstimate(flops=2 * tok * cols * wide, bytes_accessed=2 * cols * (wide + tok), transcendentals=0),
        name="unproject",
    )(table, pair, *[slots3] * per, *more)


def ring_reduce(ring, plan, tok_pair, pair, pair_both, side, finish):
    f32, bf16 = jnp.float32, jnp.bfloat16
    width = pair_both.shape[1]
    streams = 2 if width % 512 == 0 else 1
    w = width // streams
    wr = ring.win * BR
    base = ring.slots * BR
    got = [jnp.zeros(((ring.cap + ring.depth) * BR, w), bf16) for _ in range(streams)]
    near = ring.cap * BR
    group = 2 if ring.steps % 2 == 0 else 1
    rhs = [pair_both[:, i * w:(i + 1) * w] for i in range(streams)]
    chunk = [None] * streams
    aside = None
    for s in range(ring.steps - 1, -1, -1):
        first = s == ring.steps - 1
        at = (s % group) * wr
        for i in range(streams):
            if (s + 1) % group == 0:
                lo = base + (s + 1 - group) * wr
                chunk[i] = jnp.dot(tok_pair[lo:lo + group * wr], rhs[i], preferred_element_type=f32).astype(bf16)
            sent = chunk[i][at:at + wr]
            if not first:
                here = got[i][near + s * wr:near + (s + 1) * wr]
                sent = (sent.astype(f32) + here.astype(f32)).astype(bf16)
            moved = lax.ppermute(sent, "dp", ring.reduce_hop)
            if first and i == 0:
                ready, moved = lax.optimization_barrier((pair, moved))
                aside = side(ready)
            got[i] = lax.dynamic_update_slice(got[i], moved, ((ring.cap - plan["nv"] + ring.win * s) * BR, 0))
            if (s % group) == 0 and s > 0:
                extra = [aside] if s == ring.steps - group and i == 0 else []
                tied = lax.optimization_barrier((rhs[i], moved, *extra))
                rhs[i] = tied[0]
                if extra:
                    aside = finish(tied[2])
    far = [lax.ppermute(pick_blocks(plan["other"], g), "dp", ring.core_swap) for g in got]
    return emit_blocks(plan["own"], tok_pair, rhs, got, far), aside


def local(tokens, queries, out_grad, segment_ids, weight_slots, old_place, new_place):
    tok, feats = tokens.shape
    slot_rows, heads, _, hd = weight_slots.shape
    wide = heads * 2 * hd
    dp, mp = lax.axis_size("dp"), lax.axis_size("mp")
    slots = slot_rows // BR
    slot_total = dp * slots
    blocks = old_place.shape[0]
    f32, bf16 = jnp.float32, jnp.bfloat16
    q2d = queries.reshape(tok, -1)
    g2d = out_grad.reshape(tok, -1)
    cos, sin = rope_tables(tok, hd)
    segc, segr = seg_tables(segment_ids[0])

    gathered = lax.all_gather(weight_slots.reshape(slot_rows, wide), "dp", axis=0, tiled=True)

    ring = Ring(dp, slots, blocks)
    plan = ring.plan(new_place)
    tok_t = tokens.T
    tok_here = pick_blocks(plan["here"], tok_t)
    tok_there = lax.ppermute(pick_blocks(plan["there"], tok_t), "dp", ring.core_swap)
    tok_pair = jnp.concatenate([tok_here, tok_there], axis=1)

    slots3 = gathered.reshape(slot_total, BR, wide)
    proj = project(old_place, tokens, slots3)
    dq, pair = attention(proj, cos, sin, segc, segr, q2d, g2d, hd)

    def feature_part(pair):
        if mp == 2:
            half = blocks // 2
            away = lax.dynamic_slice(old_place, ((1 - lax.axis_index("mp")) * half,), (half,))
            return unproject(away, pair, slots3)
        return unproject(old_place, pair, slots3)

    def feature_carry(part):
        if mp == 2:
            return lax.ppermute(part, "mp", [(0, 1), (1, 0)])
        return lax.psum_scatter(part, "mp", scatter_dimension=1, tiled=True)

    def feature_end(pair, got):
        if mp == 2:
            half = blocks // 2
            home = lax.dynamic_slice(old_place, (lax.axis_index("mp") * half,), (half,))
            return unproject(home, pair, slots3, got)
        return got

    def fast(tok_pair, tok_t, pair, dq, slots3):
        far = lax.ppermute(pair, "dp", ring.core_swap)
        both = jnp.concatenate([pair, far], axis=0)
        wg, got = ring_reduce(ring, plan, tok_pair, pair, both, feature_part, feature_carry)
        return feature_end(pair, got), dq.reshape(queries.shape), wg.reshape(slot_rows, heads, 2, hd)

    def slow(tok_pair, tok_t, pair, dq, slots3):
        part = lax.map(lambda t: jnp.dot(t, pair, preferred_element_type=f32).astype(bf16), tok_t.reshape(blocks, BR, tok)).reshape(blocks * BR, wide)
        hit = new_place[None, :] == jnp.arange(slot_total, dtype=jnp.int32)[:, None]
        slot_block = jnp.max(jnp.where(hit, jnp.arange(blocks, dtype=jnp.int32)[None, :], -1), axis=1)
        wg = lax.psum_scatter(pick_blocks(slot_block, part), "dp", scatter_dimension=0, tiled=True).astype(f32)
        nt = (((1,), (1,)), ((), ()))
        feat = lax.map(lambda b: lax.dot_general(pair, slots3[b], nt, preferred_element_type=f32).astype(bf16), old_place)
        feat = jnp.swapaxes(feat, 0, 1).reshape(tok, feats)
        return lax.psum_scatter(feat, "mp", scatter_dimension=1, tiled=True), dq.reshape(queries.shape), wg.reshape(slot_rows, heads, 2, hd)

    return lax.cond(plan["ok"], fast, slow, tok_pair, tok_t, pair, dq, slots3)


def solution(mesh):
    return jax.shard_map(
        local,
        mesh=mesh,
        in_specs=(
            P("dp", None),
            P("dp", "mp", None),
            P("dp", "mp", None),
            P("dp", None),
            P("dp", "mp", None, None),
            P(),
            P(),
        ),
        out_specs=(P("dp", "mp"), P("dp", "mp", None), P("dp", "mp", None, None)),
        check_vma=False,
    )
```
